32 devices in a mesh: pw: 8 (over z, x), band: 4 (over y, core).
Axes of the slice: x: 2, y: 2, z: 4, core: 2. Of those that a mesh axis runs over, the one named last changes fastest.
Arguments:
- basis_set: bfloat16 [24576, 2048], P('pw'), may hold values from -0.0546875 to 0.0546875
- densities: bfloat16 [24576, 4096], P('pw', 'band'), may hold values from -135 to 135
- pair_gaps: float32 [4096], P('band'), may hold values from 0.002 to 500
- frequencies: float32 [16], replicated, may hold values from 0.01 to 100
Outputs:
- polarizability: float32 [16, 2048, 2048], P(None, 'pw', 'band')
- projected: bfloat16 [2048, 4096], P('pw', 'band')
The draws below stay inside these ranges and needn't reach their ends.
All inputs are finite; a program needn't handle non-finite values.
Results may differ from the reference program's by a relative error of at most 0.011.
Values may be sent and summed in bfloat16 or wider, within the bound.
No kernel may reach another device: no remote copies, remote signals or barrier semaphores. Data moves between devices by JAX's collectives and lax.ppermute only.
A program may use at most 128 MiB of HBM per device.

```python
import jax
import jax.numpy as jnp
from jax import lax

NPW = 24576
NB = 2048
NFREQ = 16
PAIRS = 4096


def shared_gaps(key):
    unit_draw = jax.random.uniform(jax.random.fold_in(key, 7), (PAIRS,), jnp.float32)
    return 0.002 * jnp.exp(unit_draw * jnp.log(250000.0))


def draw_pair_gaps(key, part):
    return shared_gaps(key).astype(jnp.float32)


def draw_densities(key, part):
    energy_gaps = shared_gaps(key)
    inner_key = jax.random.fold_in(key, 13)
    values = jax.random.truncated_normal(inner_key, -6.0, 6.0, (NPW, PAIRS), jnp.float32)
    return (values * jnp.sqrt(energy_gaps)[None, :]).astype(jnp.bfloat16)


def draw_frequencies(key, part):
    jitter = jax.random.uniform(jax.random.fold_in(key, 19), (NFREQ,), jnp.float32)
    position = (jnp.arange(NFREQ, dtype=jnp.float32) + jitter) / NFREQ
    return (0.01 * jnp.exp(position * jnp.log(10000.0))).astype(jnp.float32)


def raised(values, rng, source, target, shards_of, factor):
    def block_of(axis_at):
        return (jnp.arange(values.shape[axis_at]) // (values.shape[axis_at] // shards_of)).reshape((-1,) + (1,) * (values.ndim - 1 - axis_at))

    first = jax.random.permutation(rng, shards_of)[block_of(target)]
    far = (block_of(target) + shards_of // 2) % shards_of
    return jnp.where((block_of(source) == first) | (block_of(source) == far), factor * values, values)


def level_of(key, dims, pieces, low, largest):
    def one(dim, blocks):
        heights = jax.random.uniform(jax.random.fold_in(jax.random.fold_in(key, 6), dim), (blocks,), jnp.float32, low / len(pieces), largest / len(pieces))
        return jnp.repeat(jnp.exp(heights), dims[dim] // blocks).reshape((-1,) + (1,) * (len(dims) - dim - 1))

    factor_of = one(*pieces[0])
    for cut in pieces[1:]:
        factor_of = factor_of * one(*cut)
    return factor_of


def bell_draw_with(key, dims, spread, bound, shards, heavy, kind=jnp.bfloat16):
    array = spread * jax.random.normal(key, dims, jnp.float32)
    if shards:
        array = array * level_of(key, dims, shards, -0.22, 0.18)
    return jnp.clip(raised(array, jax.random.fold_in(key, 3), *heavy), -bound, bound).astype(kind)


def setup_inputs(seed: int = 0) -> dict:
    keys = jax.random.split(jax.random.key(seed), 5)
    return {
        "basis_set": bell_draw_with(keys[0], (NPW, NB), NPW ** -0.5, 0.0546875, ((0, 8),), (0, 1, 8, 2.0)),
        "densities": draw_densities(jax.random.fold_in(keys[4], 71), 0),
        "pair_gaps": draw_pair_gaps(jax.random.fold_in(keys[4], 71), 0),
        "frequencies": draw_frequencies(jax.random.fold_in(keys[4], 71), 0),
    }


def reference(basis_set, densities, pair_gaps, frequencies):
    projected = lax.dot_general(basis_set, densities, (((0,), (0,)), ((), ())), preferred_element_type=jnp.float32).astype(jnp.bfloat16)
    weights = (-4.0 / PAIRS) * pair_gaps[None, :] / (pair_gaps[None, :] ** 2 + frequencies[:, None] ** 2)

    def single(weight_row):
        scaled = (weight_row[None, :] * projected.astype(jnp.float32)).astype(jnp.bfloat16)
        return jnp.dot(scaled, projected.T, preferred_element_type=jnp.float32)

    polarizability = lax.map(single, weights)
    return polarizability, projected
```

```python
import functools

import jax
import jax.numpy as jnp
from jax import lax
from jax.experimental import pallas as pl
from jax.experimental.pallas import tpu as pltpu
from jax.sharding import PartitionSpec as P

BATCH = 256
NBATCH = 4
AXES = ("pw", "band")
VMEM = pl.BlockSpec(memory_space=pltpu.VMEM)


def weigh(gap_row, frequencies, pair_total):
    return (
        -4.0 / pair_total * gap_row[None, :] / (gap_row[None, :] ** 2 + frequencies[:, None] ** 2)
    )


def scale_rows(weights, own_rows):
    return (weights[:, None, :] * own_rows.astype(jnp.float32)[None, :, :]).astype(jnp.bfloat16)


def plain_on_device(basis_set, densities, pair_gaps, frequencies):
    basis_width = basis_set.shape[1]
    pw_count = lax.axis_size("pw")
    band_count = lax.axis_size("band")
    row_share = basis_width // pw_count
    pair_total = pair_gaps.shape[0] * band_count
    nfreq = frequencies.shape[0]
    accumulated = jnp.zeros((nfreq, row_share, basis_width // band_count), jnp.float32)
    all_gaps = lax.all_gather(pair_gaps.reshape(NBATCH, BATCH), "band", axis=1, tiled=True)
    collected = []
    for position in range(NBATCH):
        dens_block = densities[:, position * BATCH : (position + 1) * BATCH]
        own_rows = lax.psum_scatter(
            lax.dot_general(
                basis_set, dens_block, (((0,), (0,)), ((), ())), preferred_element_type=jnp.float32
            ),
            "pw",
            scatter_dimension=0,
            tiled=True,
        ).astype(jnp.bfloat16)
        gathered = lax.all_gather(own_rows, "pw", axis=0, tiled=True)
        collected.append(own_rows)
        columns = lax.all_to_all(gathered, "band", split_axis=0, concat_axis=1, tiled=True)
        rows_all = lax.all_gather(own_rows, "band", axis=1, tiled=True)
        scaled = scale_rows(weigh(all_gaps[position], frequencies, pair_total), rows_all)
        accumulated = accumulated + jnp.einsum(
            "krp,cp->krc", scaled, columns, preferred_element_type=jnp.float32
        )
    projected = jnp.concatenate(collected, axis=1)
    return (accumulated, projected)


def project_kernel(me, dens_ref, basis_ref, *outs):
    step = pl.program_id(0)
    part = lax.dot_general(
        basis_ref[...],
        dens_ref[...],
        (((0,), (0,)), ((), ())),
        preferred_element_type=jnp.float32,
    ).astype(jnp.bfloat16)
    width = outs[0].shape[2]
    for i, out in enumerate(outs):
        out[step] = part[:, i * width : (i + 1) * width]


def project(me, basis_set, densities, block, count, width, planes, rows, own):
    depth = basis_set.shape[0]

    def basis_at(step, me):
        mine = jnp.bitwise_xor(me[0], step * 2)
        return (0, mine if own else jnp.bitwise_xor(mine, 1))

    return pl.pallas_call(
        project_kernel,
        grid_spec=pltpu.PrefetchScalarGridSpec(
            num_scalar_prefetch=1,
            grid=(planes,),
            in_specs=[
                pl.BlockSpec((depth, count * width), lambda step, me: (0, block)),
                pl.BlockSpec((depth, rows), basis_at),
            ],
            out_specs=[VMEM] * count,
        ),
        out_shape=[jax.ShapeDtypeStruct((planes, rows, width), jnp.bfloat16)] * count,
        cost_estimate=pl.CostEstimate(
            flops=2 * depth * count * width * rows * planes,
            bytes_accessed=2 * depth * (count * width + rows * planes),
            transcendentals=0,
        ),
        compiler_params=pltpu.CompilerParams(
            dimension_semantics=("arbitrary",), vmem_limit_bytes=28 << 20
        ),
        name="project",
    )(me, densities, basis_set)


def fold_kernel(kept_ref, got_ref, *outs):
    for i in range(kept_ref.shape[0]):
        total = (kept_ref[i].astype(jnp.float32) + got_ref[i].astype(jnp.float32)).astype(
            jnp.bfloat16
        )
        if kept_ref.shape[0] == 1:
            outs[0][...] = total
        else:
            outs[i % 2][i // 2] = total


def fold(kept, got):
    count, rows, width = kept.shape
    if count == 1:
        shapes = [jax.ShapeDtypeStruct((rows, width), jnp.bfloat16)]
    else:
        shapes = [jax.ShapeDtypeStruct((count // 2, rows, width), jnp.bfloat16)] * 2
    return pl.pallas_call(
        fold_kernel,
        in_specs=[VMEM] * 2,
        out_specs=[VMEM] * len(shapes),
        out_shape=shapes,
        cost_estimate=pl.CostEstimate(
            flops=count * rows * width, bytes_accessed=4 * count * rows * width, transcendentals=0
        ),
        compiler_params=pltpu.CompilerParams(vmem_limit_bytes=8 << 20),
        name="fold",
    )(kept, got)


def stack_kernel(*refs):
    for i, ref in enumerate(refs[:-1]):
        refs[-1][i] = ref[...]


def stack(pieces):
    rows, width = pieces[0].shape
    return pl.pallas_call(
        stack_kernel,
        in_specs=[VMEM] * len(pieces),
        out_specs=VMEM,
        out_shape=jax.ShapeDtypeStruct((len(pieces), rows, width), jnp.bfloat16),
        cost_estimate=pl.CostEstimate(
            flops=rows * width, bytes_accessed=4 * rows * width, transcendentals=0
        ),
        compiler_params=pltpu.CompilerParams(vmem_limit_bytes=8 << 20),
        name="stack",
    )(*pieces)


def respond_kernel(me, band, weights_ref, *rest, planes, per_step, chunk, first, halves, last):
    rows_in = rest[:planes]
    cols_in = rest[planes : planes + len(halves)]
    rest = rest[planes + len(halves) :]
    acc_ref = None if first else rest[0]
    out_ref, rows_s, weights_s, scaled_s = rest if first else rest[1:]
    rows, width = rows_in[0].shape
    step = pl.program_id(0)
    side = jnp.bitwise_and(me[0], 1)
    shift = jnp.bitwise_xor(me[0] // 2, band[0])

    @pl.when(step == 0)
    def _():
        for d in range(planes):
            slot = jnp.bitwise_xor(shift, d)
            rows_s[slot] = rows_in[d][...]
            weights_s[slot] = weights_ref[d, :, chunk * width : (chunk + 1) * width]

    for k in range(planes):
        base = rows_s[k].astype(jnp.float32)
        for f in range(per_step):
            w = weights_s[k, pl.ds(step * per_step + f, 1), :]
            scaled_s[f * rows : (f + 1) * rows, k * width : (k + 1) * width] = (w * base).astype(
                jnp.bfloat16
            )
    here = pl.ds(step * per_step, per_step)
    for cols, far in zip(cols_in, halves):
        total = None
        for k in range(planes):
            part = lax.dot_general(
                scaled_s[:, k * width : (k + 1) * width],
                cols[k],
                (((1,), (1,)), ((), ())),
                preferred_element_type=jnp.float32,
            )
            total = part if total is None else total + part
        total = total.reshape(per_step, rows, rows)
        half = 1 - side if far else side
        where = pl.ds(pl.multiple_of(half * rows, rows), rows)
        if acc_ref is not None:
            total = total + acc_ref[here, :, where]
        if last:
            out_ref[:, :, where] = total
        else:
            out_ref[here, :, where] = total
    if last and len(halves) == 1:
        half = side if halves[0] else 1 - side
        where = pl.ds(pl.multiple_of(half * rows, rows), rows)
        out_ref[:, :, where] = acc_ref[here, :, where]


def respond(me, band, weights, rows_in, cols_in, halves, acc, chunk, last):
    planes = len(rows_in)
    rows, width = rows_in[0].shape
    nfreq = weights.shape[1]
    per_step = 4
    first = acc is None
    args = [weights, *rows_in, *cols_in]
    aliases = {}
    if not first:
        args.append(acc)
        if not last:
            aliases = {len(args) + 1: 0}
    if last:
        out_spec = pl.BlockSpec((per_step, rows, 2 * rows), lambda step, me, band: (step, 0, 0))
    else:
        out_spec = VMEM
    return pl.pallas_call(
        functools.partial(
            respond_kernel,
            planes=planes,
            per_step=per_step,
            chunk=chunk,
            first=first,
            halves=halves,
            last=last,
        ),
        grid_spec=pltpu.PrefetchScalarGridSpec(
            num_scalar_prefetch=2,
            grid=(nfreq // per_step,),
            in_specs=[VMEM] * len(args),
            out_specs=out_spec,
            scratch_shapes=[
                pltpu.VMEM((planes, rows, width), jnp.bfloat16),
                pltpu.VMEM((planes, nfreq, width), jnp.float32),
                pltpu.VMEM((per_step * rows, planes * width), jnp.bfloat16),
            ],
        ),
        out_shape=jax.ShapeDtypeStruct((nfreq, rows, 2 * rows), jnp.float32),
        input_output_aliases=aliases,
        cost_estimate=pl.CostEstimate(
            flops=2 * nfreq * rows * rows * len(halves) * planes * width,
            bytes_accessed=nfreq * rows * 2 * rows * 4,
            transcendentals=0,
        ),
        compiler_params=pltpu.CompilerParams(
            dimension_semantics=("arbitrary",), vmem_limit_bytes=20 << 20
        ),
        name="respond",
    )(me, band, *args)


def grid_on_device(basis_set, densities, pair_gaps, frequencies):
    planes = lax.axis_size("band")
    rows = basis_set.shape[1] // lax.axis_size("pw")
    pairs = densities.shape[1]
    width = pairs // NBATCH
    chunks = [NBATCH - 1, *range(NBATCH - 1)]

    def permute(value, move):
        pairs_of = []
        for z in range(planes):
            for x in range(2):
                for b in range(planes):
                    tz, tx, tb = move(z, x, b)
                    pairs_of.append(((z * 2 + x) * planes + b, (tz * 2 + tx) * planes + tb))
        return lax.ppermute(value, AXES, pairs_of)

    def swap(z, x, b):
        return (z, 1 - x, b)

    me = lax.axis_index("pw").astype(jnp.int32).reshape(1)
    band = lax.axis_index("band").astype(jnp.int32).reshape(1)

    def projects(block, count, own):
        return project(
            me, basis_set, densities, block, count, width, planes, rows, own
        )

    away = projects(NBATCH - 1, 1, False) + projects(0, NBATCH - 1, False)
    kept = projects(NBATCH - 1, 1, True) + projects(0, NBATCH - 1, True)
    gaps = [pair_gaps.reshape(-1, 128)]
    for d in range(1, planes):
        gaps.append(permute(gaps[0], lambda z, x, b, d=d: (z, x, b ^ d)))
    weights = jnp.stack(
        [weigh(g.reshape(-1), frequencies, pairs * planes) for g in gaps]
    )

    acc = None
    collected = [None] * NBATCH
    for i, chunk in enumerate(chunks):
        got = permute(away[i], swap)
        held, sent = fold(kept[i], got)
        got = permute(sent, lambda z, x, b: (z ^ 1, x, b))
        held, sent = fold(held, got)
        got = permute(sent, lambda z, x, b: (z ^ 2, x, b))
        (own,) = fold(held, got)
        collected[chunk] = own
        near = [permute(own, lambda z, x, b, k=k: (b ^ k, x, z)) for k in range(planes)]
        rows_in = [own] + [
            permute(own, lambda z, x, b, d=d: (z, x, b ^ d))
            for d in range(1, planes)
        ]
        near = stack(near)
        far = permute(near, swap)
        if i < NBATCH - 1:
            acc = respond(me, band, weights, rows_in, [near, far], (False, True), acc, chunk, False)
        else:
            acc = respond(me, band, weights, rows_in, [near], (False,), acc, chunk, False)
            acc = respond(me, band, weights, rows_in, [far], (True,), acc, chunk, True)
    return (acc, jnp.concatenate(collected, axis=1))


def solution(mesh):
    planes = mesh.shape["band"]
    on_grid = mesh.shape["pw"] == 2 * planes and planes == 4
    in_specs = (P("pw", None), P("pw", "band"), P("band"), P())
    out_specs = (P(None, "pw", "band"), P("pw", "band"))
    return jax.shard_map(
        grid_on_device if on_grid else plain_on_device,
        mesh=mesh,
        in_specs=in_specs,
        out_specs=out_specs,
        check_vma=False,
    )
```

```python
import functools

import jax
import jax.numpy as jnp
from jax import lax
from jax.experimental import pallas as pl
from jax.experimental.pallas import tpu as pltpu
from jax.sharding import PartitionSpec as P

BATCH = 256
NBATCH = 4
AXES = ("pw", "band")
VMEM = pl.BlockSpec(memory_space=pltpu.VMEM)


def weigh(gap_row, frequencies, pair_total):
    return (
        -4.0 / pair_total * gap_row[None, :] / (gap_row[None, :] ** 2 + frequencies[:, None] ** 2)
    )


def scale_rows(weights, own_rows):
    return (weights[:, None, :] * own_rows.astype(jnp.float32)[None, :, :]).astype(jnp.bfloat16)


def plain_on_device(basis_set, densities, pair_gaps, frequencies):
    basis_width = basis_set.shape[1]
    pw_count = lax.axis_size("pw")
    band_count = lax.axis_size("band")
    row_share = basis_width // pw_count
    pair_total = pair_gaps.shape[0] * band_count
    nfreq = frequencies.shape[0]
    accumulated = jnp.zeros((nfreq, row_share, basis_width // band_count), jnp.float32)
    all_gaps = lax.all_gather(pair_gaps.reshape(NBATCH, BATCH), "band", axis=1, tiled=True)
    collected = []
    for position in range(NBATCH):
        dens_block = densities[:, position * BATCH : (position + 1) * BATCH]
        own_rows = lax.psum_scatter(
            lax.dot_general(
                basis_set, dens_block, (((0,), (0,)), ((), ())), preferred_element_type=jnp.float32
            ),
            "pw",
            scatter_dimension=0,
            tiled=True,
        ).astype(jnp.bfloat16)
        gathered = lax.all_gather(own_rows, "pw", axis=0, tiled=True)
        collected.append(own_rows)
        columns = lax.all_to_all(gathered, "band", split_axis=0, concat_axis=1, tiled=True)
        rows_all = lax.all_gather(own_rows, "band", axis=1, tiled=True)
        scaled = scale_rows(weigh(all_gaps[position], frequencies, pair_total), rows_all)
        accumulated = accumulated + jnp.einsum(
            "krp,cp->krc", scaled, columns, preferred_element_type=jnp.float32
        )
    projected = jnp.concatenate(collected, axis=1)
    return (accumulated, projected)


def project_kernel(me, dens_ref, basis_ref, out, *flipped, offset, masks, sent):
    count, rows, width = out.shape
    if flipped:
        flipped[0][...] = dens_ref[:, offset : offset + width].T
        dens_ref = flipped[0]
    for step in range(count):
        away = (step % 2) * masks[1] + (step // 2) * masks[2] + (masks[0] if sent else 0)
        block = jnp.bitwise_xor(me[0], away)
        part = jnp.dot(
            dens_ref[...],
            basis_ref[:, pl.ds(pl.multiple_of(block * rows, rows), rows)],
            preferred_element_type=jnp.float32,
        )
        out[step] = part.T.astype(out.dtype)


def project(me, dens, basis, offset, width, rows, masks, sent):
    depth = basis.shape[0]
    count = basis.shape[1] // rows // 2
    shapes = [(count, rows, width)] + ([(width, depth)] if sent else [])
    return pl.pallas_call(
        functools.partial(project_kernel, offset=offset, masks=masks, sent=sent),
        grid_spec=pltpu.PrefetchScalarGridSpec(
            num_scalar_prefetch=1,
            grid=(1,),
            in_specs=[VMEM] * 2,
            out_specs=[VMEM] * len(shapes),
        ),
        out_shape=[jax.ShapeDtypeStruct(shape, jnp.bfloat16) for shape in shapes],
        cost_estimate=pl.CostEstimate(
            flops=2 * depth * width * rows * count, bytes_accessed=0, transcendentals=0
        ),
        compiler_params=pltpu.CompilerParams(vmem_limit_bytes=12 << 20),
        name="project",
    )(me, dens, basis)


def fold_kernel(kept_ref, got_ref, *outs):
    for i in range(kept_ref.shape[0]):
        total = (kept_ref[i].astype(jnp.float32) + got_ref[i].astype(jnp.float32)).astype(
            jnp.bfloat16
        )
        if kept_ref.shape[0] == 1:
            outs[0][...] = total
        else:
            outs[i % 2][i // 2] = total


def fold(kept, got):
    count, rows, width = kept.shape
    if count == 1:
        shapes = [jax.ShapeDtypeStruct((rows, width), jnp.bfloat16)]
    else:
        shapes = [jax.ShapeDtypeStruct((count // 2, rows, width), jnp.bfloat16)] * 2
    return pl.pallas_call(
        fold_kernel,
        in_specs=[VMEM] * 2,
        out_specs=[VMEM] * len(shapes),
        out_shape=shapes,
        cost_estimate=pl.CostEstimate(
            flops=count * rows * width, bytes_accessed=4 * count * rows * width, transcendentals=0
        ),
        compiler_params=pltpu.CompilerParams(vmem_limit_bytes=8 << 20),
        name="fold",
    )(kept, got)


def join_kernel(*refs):
    offset = 0
    for ref in refs[:-1]:
        if len(ref.shape) == 2:
            refs[-1][offset] = ref[...]
            offset += 1
        else:
            refs[-1][offset : offset + ref.shape[0]] = ref[...]
            offset += ref.shape[0]


def join(*pieces):
    rows, width = pieces[0].shape[-2:]
    count = sum(1 if p.ndim == 2 else p.shape[0] for p in pieces)
    return pl.pallas_call(
        join_kernel,
        in_specs=[VMEM] * len(pieces),
        out_specs=VMEM,
        out_shape=jax.ShapeDtypeStruct((count, rows, width), jnp.bfloat16),
        cost_estimate=pl.CostEstimate(
            flops=rows * width, bytes_accessed=4 * rows * width, transcendentals=0
        ),
        compiler_params=pltpu.CompilerParams(vmem_limit_bytes=8 << 20),
        name="join",
    )(*pieces)


def align_kernel(me, band, a_ref, b_ref, out_ref):
    plane = me[0] // 2
    turned = jnp.bitwise_and(plane, 1) * 2 + plane // 2
    shift = jnp.bitwise_xor(turned, band[0])
    for i in range(4):
        ref = a_ref if i < 2 else b_ref
        out_ref[jnp.bitwise_xor(shift, i)] = ref[i % 2]


def align(me, band, a, b):
    shape = (2 * a.shape[0], *a.shape[1:])
    return pl.pallas_call(
        align_kernel,
        grid_spec=pltpu.PrefetchScalarGridSpec(
            num_scalar_prefetch=2, grid=(1,), in_specs=[VMEM] * 2, out_specs=VMEM
        ),
        out_shape=jax.ShapeDtypeStruct(shape, a.dtype),
        cost_estimate=pl.CostEstimate(
            flops=a.size, bytes_accessed=8 * a.size, transcendentals=0
        ),
        compiler_params=pltpu.CompilerParams(vmem_limit_bytes=8 << 20),
        name="align",
    )(me, band, a, b)


def sort_kernel(me, band, two_ref, got_ref, own_ref, keep_ref, send_ref):
    other = jnp.bitwise_and(jnp.bitwise_xor(me[0] // 2, band[0]), 1)
    count = keep_ref.shape[0]

    @pl.when(other == 0)
    def _():
        keep_ref[...] = two_ref[...]
        send_ref[:count] = got_ref[...]

    @pl.when(other != 0)
    def _():
        keep_ref[...] = got_ref[...]
        send_ref[:count] = two_ref[...]

    send_ref[count] = own_ref[...]


def sort(me, band, two, got, own):
    count, rows, width = two.shape
    return pl.pallas_call(
        sort_kernel,
        grid_spec=pltpu.PrefetchScalarGridSpec(
            num_scalar_prefetch=2, grid=(1,), in_specs=[VMEM] * 3, out_specs=[VMEM] * 2
        ),
        out_shape=[
            jax.ShapeDtypeStruct((count, rows, width), two.dtype),
            jax.ShapeDtypeStruct((count + 1, rows, width), two.dtype),
        ],
        cost_estimate=pl.CostEstimate(
            flops=two.size, bytes_accessed=8 * two.size, transcendentals=0
        ),
        compiler_params=pltpu.CompilerParams(vmem_limit_bytes=8 << 20),
        name="sort",
    )(me, band, two, got, own)


def split_kernel(me, band, keep_ref, got_ref, own_ref, near_ref, send_ref, rows_ref):
    mine = jnp.bitwise_xor(me[0] // 4, band[0] // 2)
    near_ref[0] = keep_ref[mine]
    near_ref[1] = got_ref[mine]
    send_ref[0] = keep_ref[1 - mine]
    send_ref[1] = got_ref[1 - mine]
    rows_ref[0] = own_ref[...]
    rows_ref[1] = got_ref[2]


def split(me, band, keep, got, own):
    shape = jax.ShapeDtypeStruct(keep.shape, keep.dtype)
    return pl.pallas_call(
        split_kernel,
        grid_spec=pltpu.PrefetchScalarGridSpec(
            num_scalar_prefetch=2, grid=(1,), in_specs=[VMEM] * 3, out_specs=[VMEM] * 3
        ),
        out_shape=[shape] * 3,
        cost_estimate=pl.CostEstimate(
            flops=keep.size, bytes_accessed=8 * keep.size, transcendentals=0
        ),
        compiler_params=pltpu.CompilerParams(vmem_limit_bytes=8 << 20),
        name="split",
    )(me, band, keep, got, own)


def respond_kernel(me, weights_ref, rows_ref, *rest, per_step, offset, halves, acc, last):
    cols_in = rest[: len(halves)]
    rest = rest[len(halves) :]
    acc_ref = rest[0] if acc else None
    out_ref, scaled_s = rest[-2:]
    planes, rows, width = rows_ref.shape
    step = pl.program_id(0)
    side = jnp.bitwise_and(me[0], 1)
    for k in range(planes):
        base = rows_ref[k].astype(jnp.float32)
        for f in range(per_step):
            w = weights_ref[k, pl.ds(step * per_step + f, 1), offset : offset + width]
            scaled_s[f * rows : (f + 1) * rows, k * width : (k + 1) * width] = (w * base).astype(
                jnp.bfloat16
            )
    here = pl.ds(step * per_step, per_step)
    for cols, far in zip(cols_in, halves):
        total = None
        for k in range(planes):
            part = lax.dot_general(
                scaled_s[:, k * width : (k + 1) * width],
                cols[k],
                (((1,), (1,)), ((), ())),
                preferred_element_type=jnp.float32,
            )
            total = part if total is None else total + part
        total = total.reshape(per_step, rows, rows)
        half = 1 - side if far else side
        where = pl.ds(pl.multiple_of(half * rows, rows), rows)
        if acc:
            total = total + acc_ref[here, :, where]
        if last:
            out_ref[...] = total
        else:
            out_ref[here, :, where] = total


def respond(me, weights, rows_in, cols_in, halves, acc, offset, last=False, onto=None):
    planes, rows, width = rows_in.shape
    nfreq = weights.shape[1]
    per_step = 4
    args = [weights, rows_in, *cols_in]
    in_specs = [VMEM] * len(args)
    aliases = {}
    if acc is not None:
        args.append(acc)
        in_specs.append(VMEM)
        if not last:
            aliases = {len(args): 0}
    if onto is not None:
        args.append(onto)
        in_specs.append(pl.BlockSpec(memory_space=pl.ANY))
        aliases = {len(args): 0}
    if last:
        far = int(halves[0])
        out_spec = pl.BlockSpec(
            (per_step, rows, rows),
            lambda step, me: (step, 0, jnp.bitwise_xor(jnp.bitwise_and(me[0], 1), far)),
        )
    else:
        out_spec = VMEM
    return pl.pallas_call(
        functools.partial(
            respond_kernel,
            per_step=per_step,
            offset=offset,
            halves=halves,
            acc=acc is not None,
            last=last,
        ),
        grid_spec=pltpu.PrefetchScalarGridSpec(
            num_scalar_prefetch=1,
            grid=(nfreq // per_step,),
            in_specs=in_specs,
            out_specs=out_spec,
            scratch_shapes=[pltpu.VMEM((per_step * rows, planes * width), jnp.bfloat16)],
        ),
        out_shape=jax.ShapeDtypeStruct((nfreq, rows, 2 * rows), jnp.float32),
        input_output_aliases=aliases,
        cost_estimate=pl.CostEstimate(
            flops=2 * nfreq * rows * rows * len(halves) * planes * width,
            bytes_accessed=nfreq * rows * 2 * rows * 4,
            transcendentals=0,
        ),
        compiler_params=pltpu.CompilerParams(
            dimension_semantics=("arbitrary",), vmem_limit_bytes=20 << 20
        ),
        name="respond",
    )(me, *args)


def grid_on_device(basis_set, densities, pair_gaps, frequencies):
    planes = lax.axis_size("band")
    rows = basis_set.shape[1] // lax.axis_size("pw")
    pairs = densities.shape[1]
    unit = pairs // sum(SHARES)
    widths = [share * unit for share in SHARES]
    offsets = [start * unit for start in STARTS]

    def permute(value, move):
        pairs_of = []
        for z in range(planes):
            for x in range(2):
                for b in range(planes):
                    to = move(z, x, b)
                    if to is not None:
                        tz, tx, tb = to
                        pairs_of.append(((z * 2 + x) * planes + b, (tz * 2 + tx) * planes + tb))
        return lax.ppermute(value, AXES, pairs_of)

    def across(mask):
        return lambda z, x, b: (z ^ (mask // 2), x ^ (mask % 2), b)

    me = lax.axis_index("pw").astype(jnp.int32).reshape(1)
    band = lax.axis_index("band").astype(jnp.int32).reshape(1)

    away, kept = [], []
    for at, width, masks in zip(offsets, widths, MASKS):
        out, flipped = project(
            me, densities, basis_set, at, width, rows, masks, True
        )
        away.append(out)
        kept += project(me, flipped, basis_set, 0, width, rows, masks, False)
    gaps = [pair_gaps.reshape(-1, 128)]
    for d in range(1, planes):
        gaps.append(permute(gaps[0], lambda z, x, b, d=d: (z, x, b ^ d)))
    weights = jnp.stack(
        [weigh(g.reshape(-1), frequencies, pairs * planes) for g in gaps]
    )

    acc = None
    collected = []
    for i in range(len(widths)):
        masks = MASKS[i]
        got = permute(away[i], across(masks[0]))
        held, sent = fold(kept[i], got)
        got = permute(sent, across(masks[1]))
        held, sent = fold(held, got)
        got = permute(sent, across(masks[2]))
        (own,) = fold(held, got)
        collected.append(own)
        if DIRECT[i]:
            got = permute(own, lambda z, x, b: (z, x, b ^ 1))
            two = join(own, got)
            got = permute(two, lambda z, x, b: (z, x, b ^ 2))
            rows_in = join(two, got)
            got = [
                permute(two, lambda z, x, b, m=m: (b % 2 * 2 + ((b // 2) ^ m), x, z))
                for m in range(2)
            ]
            near = align(me, band, *got)
        else:
            got = permute(own, across(4))
            two = join(own, got)
            got = permute(two, across(2))
            keep, send = sort(me, band, two, got, own)
            got = permute(send, lambda z, x, b: (z, x, b ^ 1))
            near, send, two = split(me, band, keep, got, own)
            got = permute(send, lambda z, x, b: (z, x, b ^ 2))
            near = join(near, got)
            got = permute(two, lambda z, x, b: (z, x, b ^ 2))
            rows_in = join(two, got)
        far = permute(near, across(1))
        if i < len(widths) - 1:
            acc = respond(
                me, weights, rows_in, [near, far], (False, True), acc, offsets[i]
            )
        else:
            half = respond(
                me, weights, rows_in, [near], (False,), acc, offsets[i], True
            )
            acc = respond(
                me, weights, rows_in, [far], (True,), acc, offsets[i], True, half
            )
    in_place = sorted(range(len(widths)), key=lambda i: offsets[i])
    return (acc, jnp.concatenate([collected[i] for i in in_place], axis=1))


SHARES = (2, 2, 2, 2)
STARTS = (0, 2, 4, 6)
MASKS = ((1, 2, 4), (1, 2, 4), (1, 2, 4), (1, 2, 4))
DIRECT = (True, True, True, True)


def solution(mesh):
    planes = mesh.shape["band"]
    on_grid = mesh.shape["pw"] == 2 * planes and planes == 4
    in_specs = (P("pw", None), P("pw", "band"), P("band"), P())
    out_specs = (P(None, "pw", "band"), P("pw", "band"))
    return jax.shard_map(
        grid_on_device if on_grid else plain_on_device,
        mesh=mesh,
        in_specs=in_specs,
        out_specs=out_specs,
        check_vma=False,
    )
```

```python
import functools

import jax
import jax.numpy as jnp
from jax import lax
from jax.experimental import pallas as pl
from jax.experimental.pallas import tpu as pltpu
from jax.sharding import PartitionSpec as P

BATCH = 256
NBATCH = 4
AXES = ("pw", "band")
VMEM = pl.BlockSpec(memory_space=pltpu.VMEM)


def weigh(gap_row, frequencies, pair_total):
    return (
        -4.0 / pair_total * gap_row[None, :] / (gap_row[None, :] ** 2 + frequencies[:, None] ** 2)
    )


def scale_rows(weights, own_rows):
    return (weights[:, None, :] * own_rows.astype(jnp.float32)[None, :, :]).astype(jnp.bfloat16)


def plain_on_device(basis_set, densities, pair_gaps, frequencies):
    basis_width = basis_set.shape[1]
    pw_count = lax.axis_size("pw")
    band_count = lax.axis_size("band")
    row_share = basis_width // pw_count
    pair_total = pair_gaps.shape[0] * band_count
    nfreq = frequencies.shape[0]
    accumulated = jnp.zeros((nfreq, row_share, basis_width // band_count), jnp.float32)
    all_gaps = lax.all_gather(pair_gaps.reshape(NBATCH, BATCH), "band", axis=1, tiled=True)
    collected = []
    for position in range(NBATCH):
        dens_block = densities[:, position * BATCH : (position + 1) * BATCH]
        own_rows = lax.psum_scatter(
            lax.dot_general(
                basis_set, dens_block, (((0,), (0,)), ((), ())), preferred_element_type=jnp.float32
            ),
            "pw",
            scatter_dimension=0,
            tiled=True,
        ).astype(jnp.bfloat16)
        gathered = lax.all_gather(own_rows, "pw", axis=0, tiled=True)
        collected.append(own_rows)
        columns = lax.all_to_all(gathered, "band", split_axis=0, concat_axis=1, tiled=True)
        rows_all = lax.all_gather(own_rows, "band", axis=1, tiled=True)
        scaled = scale_rows(weigh(all_gaps[position], frequencies, pair_total), rows_all)
        accumulated = accumulated + jnp.einsum(
            "krp,cp->krc", scaled, columns, preferred_element_type=jnp.float32
        )
    projected = jnp.concatenate(collected, axis=1)
    return (accumulated, projected)


def head_kernel(me, dens_ref, basis_ref, out):
    out[pl.program_id(0)] = lax.dot_general(
        basis_ref[...],
        dens_ref[...],
        (((0,), (0,)), ((), ())),
        preferred_element_type=jnp.float32,
    ).astype(out.dtype)


def head(me, dens, basis, offset, width, rows, masks):
    depth = basis.shape[0]
    count = basis.shape[1] // rows // 2

    def basis_at(step, me):
        away = (step % 2) * masks[1] + (step // 2) * masks[2] + masks[0]
        return (0, jnp.bitwise_xor(me[0], away))

    return pl.pallas_call(
        head_kernel,
        grid_spec=pltpu.PrefetchScalarGridSpec(
            num_scalar_prefetch=1,
            grid=(count,),
            in_specs=[
                pl.BlockSpec((depth, width), lambda step, me: (0, offset // width)),
                pl.BlockSpec((depth, rows), basis_at),
            ],
            out_specs=VMEM,
        ),
        out_shape=jax.ShapeDtypeStruct((count, rows, width), jnp.bfloat16),
        cost_estimate=pl.CostEstimate(
            flops=2 * depth * width * rows * count,
            bytes_accessed=2 * depth * (width + rows * count),
            transcendentals=0,
        ),
        compiler_params=pltpu.CompilerParams(
            dimension_semantics=("arbitrary",), vmem_limit_bytes=60 << 20
        ),
        name="head",
    )(me, dens, basis)


def project_kernel(me, dens_ref, basis_ref, out, flipped=None, *, offset, masks, sent):
    count, rows, width = out.shape
    if flipped is not None:
        flipped[...] = dens_ref[:, offset : offset + width].T
        dens_ref = flipped
    for step in range(count):
        away = (step % 2) * masks[1] + (step // 2) * masks[2] + (masks[0] if sent else 0)
        block = jnp.bitwise_xor(me[0], away)
        part = jnp.dot(
            dens_ref[...],
            basis_ref[:, pl.ds(pl.multiple_of(block * rows, rows), rows)],
            preferred_element_type=jnp.float32,
        )
        out[step] = part.T.astype(out.dtype)


def project(me, dens, basis, offset, width, rows, masks, sent, flip):
    depth = basis.shape[0]
    count = basis.shape[1] // rows // 2
    shapes = [(count, rows, width)] + ([(width, depth)] if flip else [])
    return pl.pallas_call(
        functools.partial(project_kernel, offset=offset, masks=masks, sent=sent),
        grid_spec=pltpu.PrefetchScalarGridSpec(
            num_scalar_prefetch=1,
            grid=(1,),
            in_specs=[VMEM] * 2,
            out_specs=[VMEM] * len(shapes),
        ),
        out_shape=[jax.ShapeDtypeStruct(shape, jnp.bfloat16) for shape in shapes],
        cost_estimate=pl.CostEstimate(
            flops=2 * depth * width * rows * count, bytes_accessed=0, transcendentals=0
        ),
        compiler_params=pltpu.CompilerParams(vmem_limit_bytes=12 << 20),
        name="project",
    )(me, dens, basis)


def fold_kernel(kept_ref, got_ref, *outs):
    for i in range(kept_ref.shape[0]):
        total = (kept_ref[i].astype(jnp.float32) + got_ref[i].astype(jnp.float32)).astype(
            jnp.bfloat16
        )
        if kept_ref.shape[0] == 1:
            outs[0][...] = total
        else:
            outs[i % 2][i // 2] = total


def fold(kept, got):
    count, rows, width = kept.shape
    if count == 1:
        shapes = [jax.ShapeDtypeStruct((rows, width), jnp.bfloat16)]
    else:
        shapes = [jax.ShapeDtypeStruct((count // 2, rows, width), jnp.bfloat16)] * 2
    return pl.pallas_call(
        fold_kernel,
        in_specs=[VMEM] * 2,
        out_specs=[VMEM] * len(shapes),
        out_shape=shapes,
        cost_estimate=pl.CostEstimate(
            flops=count * rows * width, bytes_accessed=4 * count * rows * width, transcendentals=0
        ),
        compiler_params=pltpu.CompilerParams(vmem_limit_bytes=8 << 20),
        name="fold",
    )(kept, got)


def join_kernel(*refs):
    offset = 0
    for ref in refs[:-1]:
        if len(ref.shape) == 2:
            refs[-1][offset] = ref[...]
            offset += 1
        else:
            refs[-1][offset : offset + ref.shape[0]] = ref[...]
            offset += ref.shape[0]


def join(*pieces):
    rows, width = pieces[0].shape[-2:]
    count = sum(1 if p.ndim == 2 else p.shape[0] for p in pieces)
    return pl.pallas_call(
        join_kernel,
        in_specs=[VMEM] * len(pieces),
        out_specs=VMEM,
        out_shape=jax.ShapeDtypeStruct((count, rows, width), jnp.bfloat16),
        cost_estimate=pl.CostEstimate(
            flops=rows * width, bytes_accessed=4 * rows * width, transcendentals=0
        ),
        compiler_params=pltpu.CompilerParams(vmem_limit_bytes=8 << 20),
        name="join",
    )(*pieces)


def turn(value):
    return jnp.bitwise_and(value, 1) * 2 + value // 2


def align_kernel(me, band, a_ref, b_ref, out_ref, *, direct):
    plane = me[0] // 2
    if not direct:
        plane = jnp.bitwise_xor(plane, band[0])
    shift = jnp.bitwise_xor(turn(plane), band[0])
    for i in range(4):
        ref = a_ref if i < 2 else b_ref
        out_ref[jnp.bitwise_xor(shift, i)] = ref[i % 2]


def align(me, band, a, b, direct):
    shape = (2 * a.shape[0], *a.shape[1:])
    return pl.pallas_call(
        functools.partial(align_kernel, direct=direct),
        grid_spec=pltpu.PrefetchScalarGridSpec(
            num_scalar_prefetch=2, grid=(1,), in_specs=[VMEM] * 2, out_specs=VMEM
        ),
        out_shape=jax.ShapeDtypeStruct(shape, a.dtype),
        cost_estimate=pl.CostEstimate(
            flops=a.size, bytes_accessed=8 * a.size, transcendentals=0
        ),
        compiler_params=pltpu.CompilerParams(vmem_limit_bytes=8 << 20),
        name="align",
    )(me, band, a, b)


def sort_kernel(band, here_ref, got_ref, send_ref, two_ref):
    two_ref[0] = here_ref[0]
    two_ref[1] = got_ref[0]
    plane = jnp.bitwise_and(band[0], 1)
    send_ref[0] = here_ref[plane]
    send_ref[1] = got_ref[plane]


def sort(band, here, got):
    shape = jax.ShapeDtypeStruct(here.shape, here.dtype)
    return pl.pallas_call(
        sort_kernel,
        grid_spec=pltpu.PrefetchScalarGridSpec(
            num_scalar_prefetch=1, grid=(1,), in_specs=[VMEM] * 2, out_specs=[VMEM] * 2
        ),
        out_shape=[shape] * 2,
        cost_estimate=pl.CostEstimate(
            flops=here.size, bytes_accessed=8 * here.size, transcendentals=0
        ),
        compiler_params=pltpu.CompilerParams(vmem_limit_bytes=8 << 20),
        name="sort",
    )(band, here, got)


def respond_kernel(me, weights_ref, rows_ref, *rest, per_step, offset, halves, acc, last):
    cols_in = rest[: len(halves)]
    rest = rest[len(halves) :]
    acc_ref = rest[0] if acc else None
    out_ref, scaled_s = rest[-2:]
    planes, rows, width = rows_ref.shape
    step = pl.program_id(0)
    side = jnp.bitwise_and(me[0], 1)
    for k in range(planes):
        base = rows_ref[k].astype(jnp.float32)
        for f in range(per_step):
            w = weights_ref[k, pl.ds(step * per_step + f, 1), offset : offset + width]
            scaled_s[f * rows : (f + 1) * rows, k * width : (k + 1) * width] = (w * base).astype(
                jnp.bfloat16
            )
    here = pl.ds(step * per_step, per_step)
    for cols, far in zip(cols_in, halves):
        total = None
        for k in range(planes):
            part = lax.dot_general(
                scaled_s[:, k * width : (k + 1) * width],
                cols[k],
                (((1,), (1,)), ((), ())),
                preferred_element_type=jnp.float32,
            )
            total = part if total is None else total + part
        total = total.reshape(per_step, rows, rows)
        half = 1 - side if far else side
        where = pl.ds(pl.multiple_of(half * rows, rows), rows)
        if acc:
            total = total + acc_ref[here, :, where]
        if last:
            out_ref[...] = total
        else:
            out_ref[here, :, where] = total


def respond(me, weights, rows_in, cols_in, halves, acc, offset, last=False, onto=None):
    planes, rows, width = rows_in.shape
    nfreq = weights.shape[1]
    per_step = 4
    args = [weights, rows_in, *cols_in]
    in_specs = [VMEM] * len(args)
    aliases = {}
    if acc is not None:
        args.append(acc)
        in_specs.append(VMEM)
        if not last:
            aliases = {len(args): 0}
    if onto is not None:
        args.append(onto)
        in_specs.append(pl.BlockSpec(memory_space=pl.ANY))
        aliases = {len(args): 0}
    if last:
        far = int(halves[0])
        out_spec = pl.BlockSpec(
            (per_step, rows, rows),
            lambda step, me: (step, 0, jnp.bitwise_xor(jnp.bitwise_and(me[0], 1), far)),
        )
    else:
        out_spec = VMEM
    return pl.pallas_call(
        functools.partial(
            respond_kernel,
            per_step=per_step,
            offset=offset,
            halves=halves,
            acc=acc is not None,
            last=last,
        ),
        grid_spec=pltpu.PrefetchScalarGridSpec(
            num_scalar_prefetch=1,
            grid=(nfreq // per_step,),
            in_specs=in_specs,
            out_specs=out_spec,
            scratch_shapes=[pltpu.VMEM((per_step * rows, planes * width), jnp.bfloat16)],
        ),
        out_shape=jax.ShapeDtypeStruct((nfreq, rows, 2 * rows), jnp.float32),
        input_output_aliases=aliases,
        cost_estimate=pl.CostEstimate(
            flops=2 * nfreq * rows * rows * len(halves) * planes * width,
            bytes_accessed=nfreq * rows * 2 * rows * 4,
            transcendentals=0,
        ),
        compiler_params=pltpu.CompilerParams(
            dimension_semantics=("arbitrary",), vmem_limit_bytes=20 << 20
        ),
        name="respond",
    )(me, *args)


def grid_on_device(basis_set, densities, pair_gaps, frequencies):
    planes = lax.axis_size("band")
    rows = basis_set.shape[1] // lax.axis_size("pw")
    pairs = densities.shape[1]
    unit = pairs // sum(SHARES)
    widths = [share * unit for share in SHARES]
    offsets = [start * unit for start in STARTS]

    def permute(value, move):
        pairs_of = []
        for z in range(planes):
            for x in range(2):
                for b in range(planes):
                    to = move(z, x, b)
                    if to is not None:
                        tz, tx, tb = to
                        pairs_of.append(((z * 2 + x) * planes + b, (tz * 2 + tx) * planes + tb))
        return lax.ppermute(value, AXES, pairs_of)

    def across(mask):
        return lambda z, x, b: (z ^ (mask // 2), x ^ (mask % 2), b)

    me = lax.axis_index("pw").astype(jnp.int32).reshape(1)
    band = lax.axis_index("band").astype(jnp.int32).reshape(1)

    away, kept = [], []
    for i, (at, width, masks) in enumerate(zip(offsets, widths, MASKS)):
        shape = (basis_set, at, width, rows, masks)
        if i == 0:
            out = head(me, densities, *shape)
        else:
            out, flipped = project(me, densities, *shape, True, True)
        away.append(out)
        if i == 0:
            out = project(me, densities, *shape, False, True)[0]
        else:
            (out,) = project(me, flipped, *shape, False, False)
        kept.append(out)
    gaps = pair_gaps.reshape(-1, 128)
    for bit in (1, 2):
        got = permute(gaps, lambda z, x, b, bit=bit: (z, x, b ^ bit))
        gaps = jnp.concatenate([gaps, got])
    weights = jnp.stack(
        [weigh(g, frequencies, pairs * planes) for g in gaps.reshape(planes, pairs)]
    )

    acc = None
    collected = []
    for i in range(len(widths)):
        masks = MASKS[i]
        got = permute(away[i], across(masks[0]))
        held, sent = fold(kept[i], got)
        got = permute(sent, across(masks[1]))
        held, sent = fold(held, got)
        got = permute(sent, across(masks[2]))
        (own,) = fold(held, got)
        collected.append(own)
        if DIRECT[i]:
            got = permute(own, lambda z, x, b: (z, x, b ^ 1))
            two = send = join(own, got)

            def target(z, x, b, m):
                return (b % 2 * 2 + ((b // 2) ^ m), x, z)

        else:
            got = permute(own, across(4))
            here = join(own, got)
            got = permute(here, lambda z, x, b: (z, x, b ^ 1))
            send, two = sort(band, here, got)

            def target(z, x, b, m):
                return (z ^ (b // 2) ^ m, x, z ^ (b % 2 * 2))

        got = permute(two, lambda z, x, b: (z, x, b ^ 2))
        rows_in = join(two, got)
        got = [permute(send, functools.partial(target, m=m)) for m in range(2)]
        near = align(me, band, *got, DIRECT[i])
        far = permute(near, across(1))
        if i < len(widths) - 1:
            acc = respond(
                me, weights, rows_in, [near, far], (False, True), acc, offsets[i]
            )
        else:
            half = respond(
                me, weights, rows_in, [near], (False,), acc, offsets[i], True
            )
            acc = respond(
                me, weights, rows_in, [far], (True,), acc, offsets[i], True, half
            )
    in_place = sorted(range(len(widths)), key=lambda i: offsets[i])
    projected = jnp.concatenate([collected[i] for i in in_place], axis=1)
    return (acc, projected)


SHARES = (2, 2, 2, 2)
STARTS = (0, 2, 4, 6)
MASKS = ((1, 2, 4), (1, 2, 4), (1, 2, 4), (1, 2, 4))
DIRECT = (True, True, True, True)


def solution(mesh):
    planes = mesh.shape["band"]
    on_grid = mesh.shape["pw"] == 2 * planes and planes == 4
    in_specs = (P("pw", None), P("pw", "band"), P("band"), P())
    out_specs = (P(None, "pw", "band"), P("pw", "band"))
    return jax.shard_map(
        grid_on_device if on_grid else plain_on_device,
        mesh=mesh,
        in_specs=in_specs,
        out_specs=out_specs,
        check_vma=False,
    )
```
